32 devices in a mesh: gx: 4 (over y, x), gy: 8 (over z, core).
Axes of the slice: x: 2, y: 2, z: 4, core: 2. Of those that a mesh axis runs over, the one named last changes fastest.
Arguments:
- pressure: float32 [96, 192, 256], P('gx', 'gy'), may hold values from -6 to 6
- pressure_old: float32 [96, 192, 256], P('gx', 'gy'), may hold values from -6 to 6
- speed_term: float32 [96, 192, 256], P('gx', 'gy'), may hold values from 0.03 to 0.15
- layer_width: int32 [4], replicated, may hold values from 8 to 16
- source_x: int32 [4], replicated, may hold values from 0 to 95
- source_y: int32 [4], replicated, may hold values from 0 to 191
- source_z: int32 [4], replicated, may hold values from 0 to 255
- source_amp: float32 [8, 4], replicated, may hold values from -8 to 8
- receiver_x: int32 [64], replicated, may hold values from 0 to 95
- receiver_y: int32 [64], replicated, may hold values from 0 to 191
- receiver_z: int32 [64], replicated, may hold values from 0 to 255
Outputs:
- pressure_final: float32 [96, 192, 256], P('gx', 'gy')
- traces: float32 [64, 8], replicated
- energy: float32 [8], replicated
The draws below stay inside these ranges and needn't reach their ends.
All inputs are finite; a program needn't handle non-finite values.
Results may differ from the reference program's by a relative error of at most 0.00026.
Values sent between devices are 32-bit elements; how exact they have to be, the bound alone decides.
A program may use at most 64 MiB of HBM per device.

```python
import math
import jax
import jax.numpy as jnp
from jax import lax

NZ = 256
STEPS = 8
NSRC = 4
NREC = 64
NX = 96
NY = 192


def plant(entries, key, smallest, largest):
    longest = entries.shape.index(max(entries.shape))
    spots = []
    for shift in (0, 1):
        where = [jax.random.randint(jax.random.fold_in(key, axis), (), 0, length) for axis, length in enumerate(entries.shape)]
        where[longest] = (where[longest] + shift) % entries.shape[longest]
        spots.append(tuple(where))
    return entries.at[spots[0]].set(smallest).at[spots[1]].set(largest)


def block_scale(stream_key, extent, shards, least, top_value):
    level = 1.0
    for dim, shards_of in shards:
        heights = jax.random.uniform(jax.random.fold_in(jax.random.fold_in(stream_key, 6), dim), (shards_of,), jnp.float32, least / len(shards), top_value / len(shards))
        level = level * jnp.repeat(jnp.exp(heights), extent[dim] // shards_of).reshape((-1,) + (1,) * (len(extent) - 1 - dim))
    return level


def centred(stream_key, shape, spread, limit, pieces=(), held_as=jnp.bfloat16):
    drawn = jax.random.normal(stream_key, shape, jnp.float32) * spread
    if len(pieces) > 0:
        drawn = block_scale(stream_key, shape, pieces, -0.22, 0.18) * drawn
    return jnp.clip(drawn, min=-limit, max=limit).astype(held_as)


def setup_inputs(seed: int = 0) -> dict:
    arg_keys = jax.random.split(jax.random.key(seed), 12)
    return {
        "pressure": centred(arg_keys[0], (NX, NY, NZ), 1.0, 6.0, ((0, 4), (1, 8)), jnp.float32),
        "pressure_old": centred(arg_keys[1], (NX, NY, NZ), 1.0, 6.0, ((0, 4), (1, 8)), jnp.float32),
        "speed_term": jnp.clip(jnp.exp(math.log(0.15) - 1.609438 * jax.random.uniform(arg_keys[2], (NX, NY, NZ), jnp.float32) ** block_scale(arg_keys[2], (NX, NY, NZ), ((0, 4), (1, 8)), -0.2, 0.2)), 0.03, 0.15),
        "layer_width": plant(jax.random.randint(arg_keys[3], (4,), 8, 17), jax.random.fold_in(arg_keys[3], 1), 8, 16).astype(jnp.int32),
        "source_x": plant(jax.random.randint(arg_keys[4], (NSRC,), 0, NX), jax.random.fold_in(arg_keys[4], 1), 0, NX - 1).astype(jnp.int32),
        "source_y": plant(jax.random.randint(arg_keys[5], (NSRC,), 0, NY), jax.random.fold_in(arg_keys[5], 1), 0, NY - 1).astype(jnp.int32),
        "source_z": plant(jax.random.randint(arg_keys[6], (NSRC,), 0, NZ), jax.random.fold_in(arg_keys[6], 1), 0, NZ - 1).astype(jnp.int32),
        "source_amp": centred(arg_keys[7], (STEPS, NSRC), 2.0, 8.0, (), jnp.float32),
        "receiver_x": plant(jax.random.randint(arg_keys[8], (NREC,), 0, NX), jax.random.fold_in(arg_keys[8], 1), 0, NX - 1).astype(jnp.int32),
        "receiver_y": plant(jax.random.randint(arg_keys[9], (NREC,), 0, NY), jax.random.fold_in(arg_keys[9], 1), 0, NY - 1).astype(jnp.int32),
        "receiver_z": plant(jax.random.randint(arg_keys[10], (NREC,), 0, NZ), jax.random.fold_in(arg_keys[10], 1), 0, NZ - 1).astype(jnp.int32),
    }


first_coef = (0.8, -0.2, 4.0 / 105.0, -1.0 / 280.0)
second_coef = (1.6, -0.2, 8.0 / 315.0, -1.0 / 560.0)
centre_coef = -205.0 / 72.0
damping = 0.6
radius = 4


def shifted(padded, axis_id, offset, length):
    return lax.slice_in_dim(padded, radius + offset, radius + offset + length, axis=axis_id)


def first_diff(padded, axis_id, length):
    summed = first_coef[0] * (shifted(padded, axis_id, 1, length) - shifted(padded, axis_id, -1, length))
    for shift_by in range(2, 5):
        summed = summed + first_coef[shift_by - 1] * (shifted(padded, axis_id, shift_by, length) - shifted(padded, axis_id, -shift_by, length))
    return summed


def second_diff(padded, axis_id, length):
    summed = centre_coef * shifted(padded, axis_id, 0, length)
    for shift_by in range(1, 5):
        summed = summed + second_coef[shift_by - 1] * (shifted(padded, axis_id, shift_by, length) + shifted(padded, axis_id, -shift_by, length))
    return summed


def profile(position, low_width, high_width, length):
    inward_low = jnp.clip((low_width - position) / low_width, 0.0, 1.0)
    inward_high = jnp.clip((position - (length - 1 - high_width)) / high_width, 0.0, 1.0)
    return jnp.exp(-damping * (inward_low * inward_low + inward_high * inward_high))


def pad_axis(field, axis_id):
    widths = [(0, 0), (0, 0), (0, 0)]
    widths[axis_id] = (radius, radius)
    return jnp.pad(field, widths)


def reference(pressure, pressure_old, speed_term, layer_width, source_x, source_y, source_z, source_amp, receiver_x, receiver_y, receiver_z):
    widths = layer_width.astype(jnp.float32)
    global_x = profile(jnp.arange(NX, dtype=jnp.int32).astype(jnp.float32), widths[0], widths[1], NX)
    global_y = profile(jnp.arange(NY, dtype=jnp.int32).astype(jnp.float32), widths[2], widths[3], NY)
    keep_x = global_x[:, None, None]
    take_x = keep_x - 1.0
    keep_y = global_y[None, :, None]
    take_y = keep_y - 1.0
    weight = 1.0 - keep_x * keep_y
    normaliser = NZ * (float(NX * NY) - jnp.sum(global_x) * jnp.sum(global_y))
    current = pressure
    previous = pressure_old
    memory_x = jnp.zeros_like(pressure)
    memory_y = jnp.zeros_like(pressure)
    zeta_x = jnp.zeros_like(pressure)
    zeta_y = jnp.zeros_like(pressure)
    energies = []
    traces = []
    for step_index in range(STEPS):
        pad_x = pad_axis(current, 0)
        pad_y = pad_axis(current, 1)
        pad_z = pad_axis(current, 2)
        grad_x = first_diff(pad_x, 0, NX)
        grad_y = first_diff(pad_y, 1, NY)
        bend_x = second_diff(pad_x, 0, NX) + first_diff(pad_axis(memory_x, 0), 0, NX)
        zeta_x = keep_x * zeta_x + take_x * bend_x
        bend_y = second_diff(pad_y, 1, NY) + first_diff(pad_axis(memory_y, 1), 1, NY)
        zeta_y = keep_y * zeta_y + take_y * bend_y
        laplace = bend_x + zeta_x + bend_y + zeta_y + second_diff(pad_z, 2, NZ)
        following = 2.0 * current - previous + speed_term * laplace
        following = following.at[source_x, source_y, source_z].add(source_amp[step_index])
        memory_x = keep_x * memory_x + take_x * grad_x
        memory_y = keep_y * memory_y + take_y * grad_y
        energies.append(jnp.sum(weight * following * following) / normaliser)
        traces.append(following[receiver_x, receiver_y, receiver_z])
        previous = current
        current = following
    return current, jnp.stack(traces, axis=1), jnp.stack(energies)
```

```python
import functools

import jax
import jax.numpy as jnp
from jax import lax
from jax.experimental import pallas as pl
from jax.experimental.pallas import tpu as pltpu
from jax.sharding import PartitionSpec as P

MESH = pl.DeviceIdType.MESH
F32 = jnp.float32
BF16 = jnp.bfloat16
first_coef = (0.8, -0.2, 4.0 / 105.0, -1.0 / 280.0)
second_coef = (1.6, -0.2, 8.0 / 315.0, -1.0 / 560.0)
centre_coef = -205.0 / 72.0
damping = 0.6
radius = 4
GROUP = 8
UNROLL = 4
scale = 0.2
first_scaled = (4.0, -1.0, 4.0 / 21.0, -1.0 / 56.0)
second_scaled = (8.0, -1.0, 8.0 / 63.0, -1.0 / 112.0)


def split(value):
    high = value.astype(BF16)
    low = (value - high.astype(F32)).astype(BF16)
    return high, low


def dot(a, b):
    return jnp.dot(a, b, preferred_element_type=F32)


def by_distance(distance, coefs, centre):
    out = jnp.where(distance == 0, centre, 0.0)
    for k in range(1, 5):
        out = jnp.where(distance == k, coefs[k - 1], out)
    return out


def profile(position, low_width, high_width, length):
    inward_low = jnp.clip((low_width - position) / low_width, 0.0, 1.0)
    inward_high = jnp.clip((position - (length - 1 - high_width)) / high_width, 0.0, 1.0)
    return jnp.exp(-damping * (inward_low * inward_low + inward_high * inward_high))


def iota(shape, dim):
    return lax.broadcasted_iota(jnp.int32, shape, dim)


def kernel(
    ngx, ngy,
    pressure, pressure_old, speed, widths_in, sx_in, sy_in, sz_in, amp_in, rx_in, ry_in, rz_in,
    out, out_traces, out_energy,
    F, SP, LAP, FH, FL, HX, HY, MX, ZX, MY, ZY,
    BZ, BD, R32, RB, ZM, PS, KX, KY, W, TR, TE, R1, R2, LAST, R3,
    widths, src_x, src_y, src_z, amp, rec_x, rec_y, rec_z, small_sem, load_sem, send_sem, recv_sem, r1_send, r1_recv, r2_send, r2_recv, r3_send, r3_recv,
):
    cx, cy, nz = pressure.shape
    nsrc, steps = amp.shape
    nrec = rec_x.shape[0]
    gx, gy = lax.axis_index("gx"), lax.axis_index("gy")
    x0, y0 = gx * cx, gy * cy
    count_x, count_y = ngx * cx, ngy * cy
    groups = cx // GROUP
    grows = GROUP * cy

    loads = [
        pltpu.make_async_copy(pressure, F.at[0, pl.ds(radius, cx)], load_sem.at[0]),
        pltpu.make_async_copy(pressure_old, F.at[1, pl.ds(radius, cx)], load_sem.at[1]),
        pltpu.make_async_copy(speed, SP, load_sem.at[2]),
    ]
    smalls = [
        pltpu.make_async_copy(src, dst, small_sem.at[n])
        for n, (src, dst) in enumerate((
            (widths_in, widths), (sx_in, src_x), (sy_in, src_y), (sz_in, src_z),
            (amp_in, amp), (rx_in, rec_x), (ry_in, rec_y), (rz_in, rec_z),
        ))
    ]
    for load in loads + smalls:
        load.start()

    HY[...] = jnp.zeros_like(HY)

    barrier = pltpu.get_barrier_semaphore()
    count = ngx * ngy
    me = gx * ngy + gy

    def peer(o):
        p = lax.rem(me + o, count)
        return p, {"gx": p // ngy, "gy": lax.rem(p, ngy)}

    def greet(o, c):
        pl.semaphore_signal(barrier, inc=1, device_id=peer(o)[1], device_id_type=MESH)
        return c

    lax.fori_loop(1, count, greet, 0)
    pl.semaphore_wait(barrier, count - 1)

    def halos(s):
        f = F.at[s]

        def send(k, src, dst, target):
            return pltpu.make_async_remote_copy(
                src_ref=src, dst_ref=dst, send_sem=send_sem.at[k], recv_sem=recv_sem.at[s, k],
                device_id=target, device_id_type=MESH,
            )

        return (
            (gx < ngx - 1, gx > 0, send(0, f.at[pl.ds(cx, radius)], HX.at[s, 0], {"gx": gx + 1})),
            (gx > 0, gx < ngx - 1, send(1, f.at[pl.ds(radius, radius)], HX.at[s, 1], {"gx": gx - 1})),
            (gy < ngy - 1, gy > 0, send(2, f.at[pl.ds(radius, cx), pl.ds(cy - radius, radius)],
                                        HY.at[s, :, pl.ds(0, radius)], {"gy": gy + 1})),
            (gy > 0, gy < ngy - 1, send(3, f.at[pl.ds(radius, cx), pl.ds(0, radius)],
                                        HY.at[s, :, pl.ds(radius, radius)], {"gy": gy - 1})),
        )

    upper_first = lax.rem(gx, 2) == 1

    def start_sends(s):
        h = halos(s)

        def go(k):
            @pl.when(h[k][0])
            def _():
                h[k][2].start()

        @pl.when(upper_first)
        def _():
            go(0)
            go(1)

        @pl.when(jnp.logical_not(upper_first))
        def _():
            go(1)
            go(0)

        go(2)
        go(3)

    loads[0].wait()
    start_sends(0)

    for s in range(2):
        F[s, 0:radius] = jnp.zeros((radius, cy, nz), F32)
        F[s, cx + radius:cx + 2 * radius] = jnp.zeros((radius, cy, nz), F32)
        MX[s] = jnp.zeros(MX.shape[1:], F32)
    ZX[...] = jnp.zeros_like(ZX)
    MY[...] = jnp.zeros_like(MY)
    ZY[...] = jnp.zeros_like(ZY)

    z_diff = iota((nz, nz), 0) - iota((nz, nz), 1)
    BZ[...] = by_distance(jnp.abs(z_diff), second_scaled, 0.0).astype(BF16)

    def block_of(index, size):
        return jnp.floor((index.astype(F32) + 0.5) * (1.0 / size)).astype(jnp.int32)

    row, col = iota((grows, grows), 0), iota((grows, grows), 1)
    same = block_of(row, cy) == block_of(col, cy)
    diff = col - row
    BD[0:grows] = jnp.where(same, by_distance(jnp.abs(diff), second_scaled, 0.0), 0.0).astype(BF16)
    signed = by_distance(jnp.abs(diff), first_scaled, 0.0)
    BD[grows:2 * grows] = jnp.where(same, jnp.where(diff > 0, signed, -signed), 0.0).astype(BF16)
    for load in smalls:
        load.wait()
    w = [widths[i].astype(F32) for i in range(4)]
    KX[...] = profile((iota(KX.shape, 0) + x0).astype(F32), w[0], w[1], count_x)
    KY[...] = profile((iota(KY.shape, 0) + y0).astype(F32), w[2], w[3], count_y)
    yy, zz = iota((cy, nz), 0) + y0, iota((cy, nz), 1)
    for s in range(nsrc):
        PS[s] = jnp.where((yy == src_y[s]) & (zz == src_z[s]), 1.0, 0.0)

    def late_setup():
        for i in range(cx):
            W[i] = 1.0 - KX[i, 0:1] * KY[...]
        cells = iota((1, cx * cy), 1)
        lanes = iota((1, nz), 1)

        def one_receiver(r, carry):
            lx, ly = rec_x[r] - x0, rec_y[r] - y0
            owned = (lx >= 0) & (lx < cx) & (ly >= 0) & (ly < cy)
            cell = jnp.where(owned, lx * cy + ly, -1)
            R32[pl.ds(r, 1), :] = jnp.where(cells == cell, 1.0, 0.0)
            ZM[pl.ds(r, 1), :] = jnp.where(lanes == rec_z[r], 1.0, 0.0)
            return carry

        lax.fori_loop(0, nrec, one_receiver, 0, unroll=4)
        RB[...] = R32[...].astype(BF16)
        TR[...] = jnp.zeros_like(TR)
        TE[...] = jnp.zeros_like(TE)

    loads[1].wait()
    loads[2].wait()

    edge_x = (gx == 0) | (gx == ngx - 1)
    edge_y = (gy == 0) | (gy == ngy - 1)
    te_row, te_lane = iota(TE.shape, 0), iota(TE.shape, 1)
    tr_lane = iota(TR.shape, 1)

    def split_group(s, g):
        rows = pl.ds(g * grows, grows)
        fh, fl = split(F[s, pl.ds(radius + g * GROUP, GROUP)].reshape(grows, nz))
        FH[rows, :], FL[rows, :] = fh, fl
        return fh, fl

    def sampled():
        g = (dot(RB[...], FH[...]) + dot(RB[...], FL[...])) * ZM[...]
        return jnp.sum(g, axis=1, keepdims=True)

    def total(e):
        return jnp.sum(jnp.sum(e, axis=0, keepdims=True), axis=1, keepdims=True)

    def record(t, e):
        TE[...] = jnp.where((te_row == t) & (te_lane == nrec), total(e), TE[...])
        TR[...] = jnp.where(tr_lane == t, sampled(), TR[...])

    p8 = iota((8, nz), 0)
    up, down = [], []
    for d in range(radius):
        c = second_coef[radius - 1 - d]
        up.append(jnp.where(p8 + d < radius, c, 0.0))
        down.append(jnp.where(p8 - d >= radius, c, 0.0))

    def gather_copy(axis, buf, send, recv, slot, k, target):
        return pltpu.make_async_remote_copy(
            src_ref=TE, dst_ref=buf.at[slot], send_sem=send.at[k], recv_sem=recv.at[slot],
            device_id={axis: target}, device_id_type=MESH,
        )

    def gather_start(axis, at, n, buf, send, recv):
        buf[at] = TE[...]
        for o in range(1, n):
            gather_copy(axis, buf, send, recv, at, o, lax.rem(at + o, n)).start()

    def gather_finish(axis, at, n, buf, send, recv):
        for o in range(1, n):
            gather_copy(axis, buf, send, recv, lax.rem(at + o, n), o, lax.rem(at + o, n)).wait_recv()
        for o in range(1, n):
            gather_copy(axis, buf, send, recv, at, o, lax.rem(at + o, n)).wait_send()
        v = buf[0]
        for j in range(1, n):
            v += buf[j]
        TE[...] = v

    def step(t, carry, first_step=False):
        s = lax.rem(t, 2)
        o = 1 - s

        for g in range(groups):
            xs = pl.ds(g * GROUP, GROUP)
            fh, fl = split_group(s, g)
            sz = dot(fh, BZ[...]) + dot(fl, BZ[...])

            @pl.when(jnp.logical_not(edge_y))
            def _():
                sy = dot(BD[0:grows], fh) + dot(BD[0:grows], fl)
                LAP[xs] = (scale * (sz + sy)).reshape(GROUP, cy, nz)

            @pl.when(edge_y)
            def _():
                ky = KY[...][None]
                ty = ky - 1.0
                both = dot(BD[...], fh) + dot(BD[...], fl)
                mh, ml = split(MY[xs].reshape(grows, nz))
                dm = dot(BD[grows:2 * grows], mh) + dot(BD[grows:2 * grows], ml)
                f = F[s, pl.ds(radius + g * GROUP, GROUP)]
                bend = centre_coef * f + (scale * (both[0:grows] + dm)).reshape(GROUP, cy, nz)
                zy = ky * ZY[xs] + ty * bend
                ZY[xs] = zy
                LAP[xs] = (scale * sz).reshape(GROUP, cy, nz) + (bend - centre_coef * f) + zy
                MY[xs] = ky * MY[xs] + (ty * scale) * both[grows:2 * grows].reshape(GROUP, cy, nz)

        def second_x(i):
            v = centre_coef * F[s, radius + i]
            for k in range(1, 5):
                v += second_coef[k - 1] * (F[s, radius + i + k] + F[s, radius + i - k])
            return v

        def first(ref, i):
            v = first_coef[0] * (ref[s, radius + i + 1] - ref[s, radius + i - 1])
            for k in range(2, 5):
                v += first_coef[k - 1] * (ref[s, radius + i + k] - ref[s, radius + i - k])
            return v

        def update(edge, i, e):
            f = F[s, radius + i]
            bend = second_x(i)
            lap = LAP[i]
            if edge:
                kx = KX[i, 0:1]
                tx = kx - 1.0
                bend += first(MX, i)
                zx = kx * ZX[i] + tx * bend
                ZX[i] = zx
                lap += zx
                MX[o, radius + i] = kx * MX[s, radius + i] + tx * first(F, i)
            v = 2.0 * f - F[o, radius + i] + SP[i] * (lap + bend + (2.0 * centre_coef) * f)
            for q in range(nsrc):
                v += jnp.where(src_x[q] - x0 == i, amp[q, t], 0.0) * PS[q]
            F[o, radius + i] = v
            return e if first_step else e + W[i] * (f * f)

        def finish(edge):
            e = lax.fori_loop(0, cx, functools.partial(update, edge), jnp.zeros((cy, nz), F32), unroll=UNROLL)
            if not first_step:
                record(t - 1, e)

        @pl.when(edge_x)
        def _():
            finish(True)

        @pl.when(jnp.logical_not(edge_x))
        def _():
            finish(False)

        if first_step:
            late_setup()
        else:
            @pl.when(t == steps - 1)
            def _():
                flat = jnp.transpose(TR[...])[0:steps]
                TE[...] += jnp.concatenate([flat, jnp.zeros((steps, TE.shape[1] - nrec), F32)], axis=1)
                gather_start("gx", gx, ngx, R1, r1_send, r1_recv)

        now, later = halos(s), halos(o)
        more = t < steps - 1

        def received(k):
            @pl.when(now[k][1])
            def _():
                now[k][2].wait_recv()

        def resend(k):
            @pl.when(now[k][0])
            def _():
                now[k][2].wait_send()

            @pl.when(now[k][0] & more)
            def _():
                later[k][2].start()

        received(2)
        received(3)

        def halo_y(i, c):
            h = HY[s, i]
            v = (up[0] + down[0]) * h
            for d in range(1, radius):
                v += up[d] * pltpu.roll(h, 8 - d, 0) + down[d] * pltpu.roll(h, d, 0)
            F[o, radius + i, 0:8] += SP[i, 0:8] * jnp.where(p8 < radius, v, 0.0)
            F[o, radius + i, cy - 8:cy] += SP[i, cy - 8:cy] * jnp.where(p8 < radius, 0.0, v)
            return c

        lax.fori_loop(0, cx, halo_y, 0, unroll=4)

        def low_side():
            @pl.when(gx > 0)
            def _():
                now[0][2].wait_recv()
                for j in range(radius):
                    v = second_coef[j] * HX[s, 0, radius - 1]
                    for k in range(j + 2, 5):
                        v += second_coef[k - 1] * HX[s, 0, radius + j - k]
                    F[o, radius + j] += SP[j] * v
            resend(1)

        def high_side():
            @pl.when(gx < ngx - 1)
            def _():
                now[1][2].wait_recv()
                for j in range(radius):
                    i = cx - 1 - j
                    v = second_coef[j] * HX[s, 1, 0]
                    for k in range(j + 2, 5):
                        v += second_coef[k - 1] * HX[s, 1, k - 1 - j]
                    F[o, radius + i] += SP[i] * v
            resend(0)

        @pl.when(upper_first)
        def _():
            high_side()
            low_side()

        @pl.when(jnp.logical_not(upper_first))
        def _():
            low_side()
            high_side()

        resend(2)
        resend(3)
        return carry

    step(0, 0, True)
    lax.fori_loop(1, steps, step, 0)
    last = steps % 2
    for g in range(groups):
        split_group(last, g)

    def energy_row(i, e):
        f = F[last, radius + i]
        return e + W[i] * (f * f)

    amount = total(lax.fori_loop(0, cx, energy_row, jnp.zeros((cy, nz), F32), unroll=UNROLL))
    row = jnp.transpose(jnp.broadcast_to(sampled(), TR.shape))[0:1]
    row = jnp.concatenate([row, jnp.zeros((1, TE.shape[1] - nrec), F32)], axis=1)
    LAST[0] = jnp.where(iota(row.shape, 1) == nrec, amount, row)
    R3[me] = LAST[0]

    def last_copy(slot, o, target):
        return pltpu.make_async_remote_copy(
            src_ref=LAST, dst_ref=R3.at[pl.ds(slot, 1)], send_sem=r3_send.at[o], recv_sem=r3_recv.at[slot],
            device_id=target, device_id_type=MESH,
        )

    def last_start(o, c):
        last_copy(me, o, peer(o)[1]).start()
        return c

    def last_wait(o, c):
        p, target = peer(o)
        last_copy(p, o, target).wait_recv()
        last_copy(me, o, target).wait_send()
        return c

    lax.fori_loop(1, count, last_start, 0)
    out[...] = F[last, pl.ds(radius, cx)]
    gather_finish("gx", gx, ngx, R1, r1_send, r1_recv)
    gather_start("gy", gy, ngy, R2, r2_send, r2_recv)
    def total_of(count, low, high):
        return jnp.sum(profile(iota((1, count), 1).astype(F32), low, high, count), axis=1, keepdims=True)

    norm = nz * (float(count_x * count_y) - total_of(count_x, w[0], w[1]) * total_of(count_y, w[2], w[3]))
    gather_finish("gy", gy, ngy, R2, r2_send, r2_recv)
    lax.fori_loop(1, count, last_wait, 0)
    final = jnp.sum(R3[...], axis=0)
    TE[...] = jnp.where(te_row == steps - 1, final, TE[...])
    out_traces[...] = TE[:, 0:nrec]
    out_energy[...] = jnp.transpose(TE[...])[nrec:nrec + 1] / norm


def store(*refs):
    sem = refs[-1]
    copies = [pltpu.make_async_copy(refs[n], refs[n + 3], sem.at[n]) for n in range(3)]
    for copy in copies:
        copy.start()
    for copy in copies:
        copy.wait()


def solution(mesh):
    ngx, ngy = mesh.shape["gx"], mesh.shape["gy"]

    def per_device(pressure, pressure_old, speed, widths, sx, sy, sz, amp, rx, ry, rz):
        cx, cy, nz = pressure.shape
        steps, nsrc = amp.shape
        nrec = rx.shape[0]
        lanes = (nrec // 128 + 1) * 128
        vmem = functools.partial(pltpu.VMEM)
        grows = GROUP * cy
        shapes = ((cx, cy, nz), (steps, nrec), (1, steps))
        held = pl.pallas_call(
            functools.partial(kernel, ngx, ngy),
            out_shape=tuple(vmem(shape, F32) for shape in shapes),
            in_specs=[pl.BlockSpec(memory_space=pltpu.HBM)] * 11,
            out_specs=(pl.BlockSpec(memory_space=pltpu.VMEM),) * 3,
            scratch_shapes=[
                vmem((2, cx + 2 * radius, cy, nz), F32),
                vmem((cx, cy, nz), F32),
                vmem((cx, cy, nz), F32),
                vmem((cx * cy, nz), BF16),
                vmem((cx * cy, nz), BF16),
                vmem((2, 2, radius, cy, nz), F32),
                vmem((2, cx, 2 * radius, nz), F32),
                vmem((2, cx + 2 * radius, cy, nz), F32),
                vmem((cx, cy, nz), F32),
                vmem((cx, cy, nz), F32),
                vmem((cx, cy, nz), F32),
                vmem((nz, nz), BF16),
                vmem((2 * grows, grows), BF16),
                vmem((nrec, cx * cy), F32),
                vmem((nrec, cx * cy), BF16),
                vmem((nrec, nz), F32),
                vmem((nsrc, cy, nz), F32),
                vmem((cx, 8, nz), F32),
                vmem((cy, nz), F32),
                vmem((cx, cy, nz), F32),
                vmem((nrec, 128), F32),
                vmem((steps, lanes), F32),
                vmem((ngx, steps, lanes), F32),
                vmem((ngy, steps, lanes), F32),
                vmem((1, 1, lanes), F32),
                vmem((ngx * ngy, 1, lanes), F32),
                pltpu.SMEM(widths.shape, jnp.int32),
                pltpu.SMEM(sx.shape, jnp.int32),
                pltpu.SMEM(sy.shape, jnp.int32),
                pltpu.SMEM(sz.shape, jnp.int32),
                pltpu.SMEM((nsrc, steps), F32),
                pltpu.SMEM(rx.shape, jnp.int32),
                pltpu.SMEM(ry.shape, jnp.int32),
                pltpu.SMEM(rz.shape, jnp.int32),
                pltpu.SemaphoreType.DMA((8,)),
                pltpu.SemaphoreType.DMA((3,)),
                pltpu.SemaphoreType.DMA((4,)),
                pltpu.SemaphoreType.DMA((2, 4)),
                pltpu.SemaphoreType.DMA((ngx,)),
                pltpu.SemaphoreType.DMA((ngx,)),
                pltpu.SemaphoreType.DMA((ngy,)),
                pltpu.SemaphoreType.DMA((ngy,)),
                pltpu.SemaphoreType.DMA((ngx * ngy,)),
                pltpu.SemaphoreType.DMA((ngx * ngy,)),
            ],
            compiler_params=pltpu.CompilerParams(
                collective_id=0, has_side_effects=True, vmem_limit_bytes=64 * 1024 * 1024 - 2 * 1024 * 1024
            ),
            name="wave",
        )(pressure, pressure_old, speed, widths, sx, sy, sz, amp.T, rx, ry, rz)
        final, traces, energy = pl.pallas_call(
            store,
            out_shape=tuple(jax.ShapeDtypeStruct(shape, F32) for shape in shapes),
            in_specs=[pl.BlockSpec(memory_space=pltpu.VMEM)] * 3,
            out_specs=(pl.BlockSpec(memory_space=pltpu.HBM),) * 3,
            scratch_shapes=[pltpu.SemaphoreType.DMA((3,))],
            compiler_params=pltpu.CompilerParams(has_side_effects=True, vmem_limit_bytes=1024 * 1024),
            name="store",
        )(*held)
        return final, traces.T, energy.reshape(steps)

    in_specs = (P("gx", "gy", None),) * 3 + (P(),) * 8
    out_specs = (P("gx", "gy", None), P(), P())
    return jax.shard_map(per_device, mesh=mesh, in_specs=in_specs, out_specs=out_specs, check_vma=False)
```

```python
import functools

import jax
import jax.numpy as jnp
from jax import lax
from jax.experimental import pallas as pl
from jax.experimental.pallas import tpu as pltpu
from jax.sharding import PartitionSpec as P

MESH = pl.DeviceIdType.MESH
F32 = jnp.float32
BF16 = jnp.bfloat16
centre_coef = -205.0 / 72.0
damping = 0.6
radius = 4
GROUP = 8
UNROLL = 4
scale = 0.2
centre_scaled = centre_coef / scale
first_scaled = (4.0, -1.0, 4.0 / 21.0, -1.0 / 56.0)
second_scaled = (8.0, -1.0, 8.0 / 63.0, -1.0 / 112.0)


def split(value):
    high = value.astype(BF16)
    low = (value - high.astype(F32)).astype(BF16)
    return high, low


def dot(a, b):
    return jnp.dot(a, b, preferred_element_type=F32)


def by_distance(distance, coefs, centre):
    out = jnp.where(distance == 0, centre, 0.0)
    for k in range(1, 5):
        out = jnp.where(distance == k, coefs[k - 1], out)
    return out


def profile(position, low_width, high_width, length):
    inward_low = jnp.clip((low_width - position) / low_width, 0.0, 1.0)
    inward_high = jnp.clip((position - (length - 1 - high_width)) / high_width, 0.0, 1.0)
    return jnp.exp(-damping * (inward_low * inward_low + inward_high * inward_high))


def iota(shape, dim):
    return lax.broadcasted_iota(jnp.int32, shape, dim)


def kernel(
    ngx, ngy,
    pressure, pressure_old, speed, widths_in, sx_in, sy_in, sz_in, amp_in, rx_in, ry_in, rz_in,
    out, out_traces, out_energy,
    F, SP, AF, LAP, FH, FL, HX, HY, MX, ZX, MY, ZY,
    BZ, BD, R32, RB, ZM, PS, KX, KY, W, TR, TE, R1, R2, LAST, R3,
    widths, src_x, src_y, src_z, amp, rec_x, rec_y, rec_z, small_sem, load_sem, x_send, x_recv, y_send, y_recv, r1_send, r1_recv, r2_send, r2_recv, r3_send, r3_recv,
):
    cx, cy, nz = pressure.shape
    nsrc, steps = amp.shape
    nrec = rec_x.shape[0]
    gx, gy = lax.axis_index("gx"), lax.axis_index("gy")
    x0, y0 = gx * cx, gy * cy
    count_x, count_y = ngx * cx, ngy * cy
    groups = cx // GROUP
    grows = GROUP * cy

    loads = [
        pltpu.make_async_copy(pressure, F.at[0, pl.ds(radius, cx)], load_sem.at[0]),
        pltpu.make_async_copy(pressure_old, F.at[1, pl.ds(radius, cx)], load_sem.at[1]),
        pltpu.make_async_copy(speed, SP, load_sem.at[2]),
    ]
    smalls = [
        pltpu.make_async_copy(src, dst, small_sem.at[n])
        for n, (src, dst) in enumerate((
            (widths_in, widths), (sx_in, src_x), (sy_in, src_y), (sz_in, src_z),
            (amp_in, amp), (rx_in, rec_x), (ry_in, rec_y), (rz_in, rec_z),
        ))
    ]
    for load in loads + smalls:
        load.start()

    HY[...] = jnp.zeros_like(HY)

    barrier = pltpu.get_barrier_semaphore()
    count = ngx * ngy
    me = gx * ngy + gy

    def peer(o):
        p = lax.rem(me + o, count)
        return p, {"gx": p // ngy, "gy": lax.rem(p, ngy)}

    near = ((gx > 0, {"gx": gx - 1}), (gx < ngx - 1, {"gx": gx + 1}), (gy > 0, {"gy": gy - 1}), (gy < ngy - 1, {"gy": gy + 1}))
    for there, who in near:
        @pl.when(there)
        def _(who=who):
            pl.semaphore_signal(barrier, inc=1, device_id=who, device_id_type=MESH)
    pl.semaphore_wait(barrier, sum(there.astype(jnp.int32) for there, _ in near))

    odd = lax.rem(gx, 2)
    pieces = cy // 8
    here_x = lambda side: jnp.where(side == 1, gx < ngx - 1, gx > 0)
    to_y = (gy < ngy - 1, gy > 0)
    from_y = (gy > 0, gy < ngy - 1)

    def x_copy(slot, side, c, arriving):
        rows = pl.ds(8 * c, 8)
        at = side if arriving else 1 - side
        return pltpu.make_async_remote_copy(
            src_ref=F.at[slot, pl.ds(radius + side * (cx - radius), radius), rows],
            dst_ref=HX.at[slot, at, :, rows],
            send_sem=x_send.at[side * pieces + c], recv_sem=x_recv.at[slot, at * pieces + c],
            device_id={"gx": gx + 2 * side - 1}, device_id_type=MESH,
        )

    def y_copy(slot, d, part, first, count_planes):
        return pltpu.make_async_remote_copy(
            src_ref=F.at[slot, pl.ds(radius + first, count_planes), pl.ds(0 if d else cy - radius, radius)],
            dst_ref=HY.at[slot, pl.ds(first, count_planes), pl.ds(radius if d else 0, radius)],
            send_sem=y_send.at[2 * part + d], recv_sem=y_recv.at[slot, 2 * part + d],
            device_id={"gy": gy - 1 if d else gy + 1}, device_id_type=MESH,
        )

    middle = (2, radius, cx - 2 * radius)

    def edge_part(side):
        return (side, side * (cx - radius), radius)

    def start_sends(slot):
        def one_side(n, c):
            side = lax.rem(n + odd, 2)

            @pl.when(here_x(side))
            def _():
                for p in range(pieces):
                    x_copy(slot, side, p, False).start()
            for d in range(2):
                @pl.when(to_y[d])
                def _(d=d):
                    y_copy(slot, d, *edge_part(side)).start()
            return c

        lax.fori_loop(0, 2, one_side, 0)
        for d in range(2):
            @pl.when(to_y[d])
            def _(d=d):
                y_copy(slot, d, *middle).start()

    loads[0].wait()
    start_sends(0)

    for s in range(2):
        F[s, 0:radius] = jnp.zeros((radius, cy, nz), F32)
        F[s, cx + radius:cx + 2 * radius] = jnp.zeros((radius, cy, nz), F32)
        MX[s] = jnp.zeros(MX.shape[1:], F32)
    ZX[...] = jnp.zeros_like(ZX)
    MY[...] = jnp.zeros_like(MY)
    ZY[...] = jnp.zeros_like(ZY)

    z_diff = iota((nz, nz), 0) - iota((nz, nz), 1)
    BZ[...] = by_distance(jnp.abs(z_diff), second_scaled, 0.0).astype(BF16)

    def block_of(index, size):
        return jnp.floor((index.astype(F32) + 0.5) * (1.0 / size)).astype(jnp.int32)

    row, col = iota((grows, grows), 0), iota((grows, grows), 1)
    same = block_of(row, cy) == block_of(col, cy)
    diff = col - row
    BD[0:grows] = jnp.where(same, by_distance(jnp.abs(diff), second_scaled, 0.0), 0.0).astype(BF16)
    signed = by_distance(jnp.abs(diff), first_scaled, 0.0)
    BD[grows:2 * grows] = jnp.where(same, jnp.where(diff > 0, signed, -signed), 0.0).astype(BF16)
    for load in smalls:
        load.wait()
    w = [widths[i].astype(F32) for i in range(4)]
    KX[...] = profile((iota(KX.shape, 0) + x0).astype(F32), w[0], w[1], count_x)
    KY[...] = profile((iota(KY.shape, 0) + y0).astype(F32), w[2], w[3], count_y)
    yy, zz = iota((cy, nz), 0) + y0, iota((cy, nz), 1)
    for s in range(nsrc):
        PS[s] = jnp.where((yy == src_y[s]) & (zz == src_z[s]), 1.0, 0.0)

    def late_setup():
        for i in range(cx):
            W[i] = 1.0 - KX[i, 0:1] * KY[...]
        cells = iota((1, cx * cy), 1)
        lanes = iota((1, nz), 1)

        def one_receiver(r, carry):
            lx, ly = rec_x[r] - x0, rec_y[r] - y0
            owned = (lx >= 0) & (lx < cx) & (ly >= 0) & (ly < cy)
            cell = jnp.where(owned, lx * cy + ly, -1)
            R32[pl.ds(r, 1), :] = jnp.where(cells == cell, 1.0, 0.0)
            ZM[pl.ds(r, 1), :] = jnp.where(lanes == rec_z[r], 1.0, 0.0)
            return carry

        lax.fori_loop(0, nrec, one_receiver, 0, unroll=4)
        RB[...] = R32[...].astype(BF16)
        TR[...] = jnp.zeros_like(TR)
        TE[...] = jnp.zeros_like(TE)

    loads[1].wait()
    loads[2].wait()

    def prescale(i, c):
        v = SP[i]
        AF[i] = 2.0 + (3.0 * centre_coef) * v
        SP[i] = scale * v
        return c

    lax.fori_loop(0, cx, prescale, 0, unroll=4)
    edge_x = (gx == 0) | (gx == ngx - 1)
    edge_y = (gy == 0) | (gy == ngy - 1)
    te_row, te_lane = iota(TE.shape, 0), iota(TE.shape, 1)
    tr_lane = iota(TR.shape, 1)

    def split_group(s, g):
        rows = pl.ds(g * grows, grows)
        fh, fl = split(F[s, pl.ds(radius + g * GROUP, GROUP)].reshape(grows, nz))
        FH[rows, :], FL[rows, :] = fh, fl
        return fh, fl

    def sampled():
        g = (dot(RB[...], FH[...]) + dot(RB[...], FL[...])) * ZM[...]
        return jnp.sum(g, axis=1, keepdims=True)

    def total(e):
        return jnp.sum(jnp.sum(e, axis=0, keepdims=True), axis=1, keepdims=True)

    def record(t, e):
        TE[...] = jnp.where((te_row == t) & (te_lane == nrec), total(e), TE[...])
        TR[...] = jnp.where(tr_lane == t, sampled(), TR[...])

    p8 = iota((8, nz), 0)
    up, down = [], []
    for d in range(radius):
        c = second_scaled[radius - 1 - d]
        up.append(jnp.where(p8 + d < radius, c, 0.0))
        down.append(jnp.where(p8 - d >= radius, c, 0.0))

    def gather_copy(axis, buf, send, recv, slot, k, target):
        return pltpu.make_async_remote_copy(
            src_ref=TE, dst_ref=buf.at[slot], send_sem=send.at[k], recv_sem=recv.at[slot],
            device_id={axis: target}, device_id_type=MESH,
        )

    def gather_start(axis, at, n, buf, send, recv):
        buf[at] = TE[...]
        for o in range(1, n):
            gather_copy(axis, buf, send, recv, at, o, lax.rem(at + o, n)).start()

    def gather_finish(axis, at, n, buf, send, recv):
        for o in range(1, n):
            gather_copy(axis, buf, send, recv, lax.rem(at + o, n), o, lax.rem(at + o, n)).wait_recv()
        for o in range(1, n):
            gather_copy(axis, buf, send, recv, at, o, lax.rem(at + o, n)).wait_send()
        v = buf[0]
        for j in range(1, n):
            v += buf[j]
        TE[...] = v

    def step(t, carry, first_step=False):
        s = lax.rem(t, 2)
        o = 1 - s

        @pl.when(jnp.logical_not(edge_y))
        def _():
            for g in range(groups):
                fh, fl = split_group(s, g)
                sums = dot(fh, BZ[...]) + dot(fl, BZ[...]) + dot(BD[0:grows], fh) + dot(BD[0:grows], fl)
                LAP[pl.ds(g * GROUP, GROUP)] = sums.reshape(GROUP, cy, nz)

        @pl.when(edge_y)
        def _():
            ky = KY[...][None]
            ty = ky - 1.0
            for g in range(groups):
                xs = pl.ds(g * GROUP, GROUP)
                fh, fl = split_group(s, g)
                sz = dot(fh, BZ[...]) + dot(fl, BZ[...])
                sy = dot(BD[0:grows], fh) + dot(BD[0:grows], fl)
                mh, ml = split(MY[xs].reshape(grows, nz))
                bend = (sy + dot(BD[grows:2 * grows], mh) + dot(BD[grows:2 * grows], ml)).reshape(GROUP, cy, nz)
                df = dot(BD[grows:2 * grows], fh) + dot(BD[grows:2 * grows], fl)
                f = F[s, pl.ds(radius + g * GROUP, GROUP)]
                zy = ky * ZY[xs] + ty * (bend + centre_scaled * f)
                ZY[xs] = zy
                LAP[xs] = sz.reshape(GROUP, cy, nz) + bend + zy
                MY[xs] = ky * MY[xs] + (scale * ty) * df.reshape(GROUP, cy, nz)

        def second_x(i):
            pair = [F[s, radius + i + k] + F[s, radius + i - k] for k in range(1, 5)]
            return second_scaled[0] * pair[0] - pair[1] + second_scaled[2] * pair[2] + second_scaled[3] * pair[3]

        def first(ref, i):
            pair = [ref[s, radius + i + k] - ref[s, radius + i - k] for k in range(1, 5)]
            return first_scaled[0] * pair[0] - pair[1] + first_scaled[2] * pair[2] + first_scaled[3] * pair[3]

        def update(edge, i, e):
            f = F[s, radius + i]
            bend = second_x(i)
            lap = LAP[i]
            if edge:
                kx = KX[i, 0:1]
                tx = kx - 1.0
                bend += first(MX, i)
                zx = kx * ZX[i] + tx * (bend + centre_scaled * f)
                ZX[i] = zx
                lap += zx
                MX[o, radius + i] = kx * MX[s, radius + i] + (scale * tx) * first(F, i)
            v = AF[i] * f - F[o, radius + i] + SP[i] * (lap + bend)
            for q in range(nsrc):
                v += jnp.where(src_x[q] - x0 == i, amp[q, t], 0.0) * PS[q]
            F[o, radius + i] = v
            return e if first_step else e + W[i] * (f * f)

        def finish(edge):
            e = lax.fori_loop(0, cx, functools.partial(update, edge), jnp.zeros((cy, nz), F32), unroll=UNROLL)
            if not first_step:
                record(t - 1, e)

        @pl.when(edge_x)
        def _():
            finish(True)

        @pl.when(jnp.logical_not(edge_x))
        def _():
            finish(False)

        if first_step:
            late_setup()
        else:
            @pl.when(t == steps - 1)
            def _():
                flat = jnp.transpose(TR[...])[0:steps]
                TE[...] += jnp.concatenate([flat, jnp.zeros((steps, TE.shape[1] - nrec), F32)], axis=1)
                gather_start("gx", gx, ngx, R1, r1_send, r1_recv)

        more = t < steps - 1

        def halo_y(part):
            _, begin, n = part
            for d in range(2):
                @pl.when(from_y[d])
                def _(d=d):
                    y_copy(s, d, *part).wait_recv()

            def one(k, c):
                i = begin + k
                h = HY[s, i]
                v = (up[0] + down[0]) * h
                for d in range(1, radius):
                    v += up[d] * pltpu.roll(h, 8 - d, 0) + down[d] * pltpu.roll(h, d, 0)
                F[o, radius + i, 0:8] += SP[i, 0:8] * jnp.where(p8 < radius, v, 0.0)
                F[o, radius + i, cy - 8:cy] += SP[i, cy - 8:cy] * jnp.where(p8 < radius, 0.0, v)
                return c

            lax.fori_loop(0, n, one, 0, unroll=4)

        def send_y(part):
            for d in range(2):
                @pl.when(to_y[d])
                def _(d=d):
                    y_copy(s, d, *part).wait_send()

                @pl.when(to_y[d] & more)
                def _(d=d):
                    y_copy(o, d, *part).start()

        halo_y(middle)
        send_y(middle)

        def one_side(n, carry):
            side = lax.rem(n + odd, 2)
            part = edge_part(side)
            halo_y(part)

            @pl.when(here_x(side))
            def _():
                for p in range(pieces):
                    rows = pl.ds(8 * p, 8)
                    x_copy(s, side, p, True).wait_recv()
                    h = [HX[s, side, jnp.where(side == 1, m, radius - 1 - m), rows] for m in range(radius)]
                    for j in range(radius):
                        i = jnp.where(side == 1, cx - 1 - j, j)
                        v = second_scaled[j] * h[0]
                        for k in range(j + 2, 5):
                            v += second_scaled[k - 1] * h[k - 1 - j]
                        F[o, radius + i, rows] += SP[i, rows] * v
                    x_copy(s, side, p, False).wait_send()

                    @pl.when(more)
                    def _():
                        x_copy(o, side, p, False).start()

            send_y(part)
            return carry

        lax.fori_loop(0, 2, one_side, 0)
        return carry

    step(0, 0, True)
    lax.fori_loop(1, steps, step, 0)
    last = steps % 2
    gather_finish("gx", gx, ngx, R1, r1_send, r1_recv)
    for g in range(groups):
        split_group(last, g)

    def energy_row(i, e):
        f = F[last, radius + i]
        return e + W[i] * (f * f)

    amount = total(lax.fori_loop(0, cx, energy_row, jnp.zeros((cy, nz), F32), unroll=UNROLL))
    row = jnp.transpose(jnp.broadcast_to(sampled(), TR.shape))[0:1]
    row = jnp.concatenate([row, jnp.zeros((1, TE.shape[1] - nrec), F32)], axis=1)
    LAST[0] = jnp.where(iota(row.shape, 1) == nrec, amount, row)
    R3[me] = LAST[0]

    def last_copy(slot, o, target):
        return pltpu.make_async_remote_copy(
            src_ref=LAST, dst_ref=R3.at[pl.ds(slot, 1)], send_sem=r3_send.at[o], recv_sem=r3_recv.at[slot],
            device_id=target, device_id_type=MESH,
        )

    def last_start(o, c):
        last_copy(me, o, peer(o)[1]).start()
        return c

    def last_wait(o, c):
        p, target = peer(o)
        last_copy(p, o, target).wait_recv()
        last_copy(me, o, target).wait_send()
        return c

    lax.fori_loop(1, count, last_start, 0)
    out[...] = F[last, pl.ds(radius, cx)]
    gather_start("gy", gy, ngy, R2, r2_send, r2_recv)
    def total_of(count, low, high):
        return jnp.sum(profile(iota((1, count), 1).astype(F32), low, high, count), axis=1, keepdims=True)

    norm = nz * (float(count_x * count_y) - total_of(count_x, w[0], w[1]) * total_of(count_y, w[2], w[3]))
    gather_finish("gy", gy, ngy, R2, r2_send, r2_recv)
    lax.fori_loop(1, count, last_wait, 0)
    final = jnp.sum(R3[...], axis=0)
    TE[...] = jnp.where(te_row == steps - 1, final, TE[...])
    out_traces[...] = TE[:, 0:nrec]
    out_energy[...] = jnp.transpose(TE[...])[nrec:nrec + 1] / norm


def store(*refs):
    sem = refs[-1]
    copies = [pltpu.make_async_copy(refs[n], refs[n + 3], sem.at[n]) for n in range(3)]
    for copy in copies:
        copy.start()
    for copy in copies:
        copy.wait()


def solution(mesh):
    ngx, ngy = mesh.shape["gx"], mesh.shape["gy"]

    def per_device(pressure, pressure_old, speed, widths, sx, sy, sz, amp, rx, ry, rz):
        cx, cy, nz = pressure.shape
        steps, nsrc = amp.shape
        nrec = rx.shape[0]
        lanes = (nrec // 128 + 1) * 128
        vmem = functools.partial(pltpu.VMEM)
        grows = GROUP * cy
        shapes = ((cx, cy, nz), (steps, nrec), (1, steps))
        held = pl.pallas_call(
            functools.partial(kernel, ngx, ngy),
            out_shape=tuple(vmem(shape, F32) for shape in shapes),
            in_specs=[pl.BlockSpec(memory_space=pltpu.HBM)] * 11,
            out_specs=(pl.BlockSpec(memory_space=pltpu.VMEM),) * 3,
            scratch_shapes=[
                vmem((2, cx + 2 * radius, cy, nz), F32),
                vmem((cx, cy, nz), F32),
                vmem((cx, cy, nz), F32),
                vmem((cx, cy, nz), F32),
                vmem((cx * cy, nz), BF16),
                vmem((cx * cy, nz), BF16),
                vmem((2, 2, radius, cy, nz), F32),
                vmem((2, cx, 2 * radius, nz), F32),
                vmem((2, cx + 2 * radius, cy, nz), F32),
                vmem((cx, cy, nz), F32),
                vmem((cx, cy, nz), F32),
                vmem((cx, cy, nz), F32),
                vmem((nz, nz), BF16),
                vmem((2 * grows, grows), BF16),
                vmem((nrec, cx * cy), F32),
                vmem((nrec, cx * cy), BF16),
                vmem((nrec, nz), F32),
                vmem((nsrc, cy, nz), F32),
                vmem((cx, 8, nz), F32),
                vmem((cy, nz), F32),
                vmem((cx, cy, nz), F32),
                vmem((nrec, 128), F32),
                vmem((steps, lanes), F32),
                vmem((ngx, steps, lanes), F32),
                vmem((ngy, steps, lanes), F32),
                vmem((1, 1, lanes), F32),
                vmem((ngx * ngy, 1, lanes), F32),
                pltpu.SMEM(widths.shape, jnp.int32),
                pltpu.SMEM(sx.shape, jnp.int32),
                pltpu.SMEM(sy.shape, jnp.int32),
                pltpu.SMEM(sz.shape, jnp.int32),
                pltpu.SMEM((nsrc, steps), F32),
                pltpu.SMEM(rx.shape, jnp.int32),
                pltpu.SMEM(ry.shape, jnp.int32),
                pltpu.SMEM(rz.shape, jnp.int32),
                pltpu.SemaphoreType.DMA((8,)),
                pltpu.SemaphoreType.DMA((3,)),
                pltpu.SemaphoreType.DMA((2 * (cy // 8),)),
                pltpu.SemaphoreType.DMA((2, 2 * (cy // 8))),
                pltpu.SemaphoreType.DMA((6,)),
                pltpu.SemaphoreType.DMA((2, 6)),
                pltpu.SemaphoreType.DMA((ngx,)),
                pltpu.SemaphoreType.DMA((ngx,)),
                pltpu.SemaphoreType.DMA((ngy,)),
                pltpu.SemaphoreType.DMA((ngy,)),
                pltpu.SemaphoreType.DMA((ngx * ngy,)),
                pltpu.SemaphoreType.DMA((ngx * ngy,)),
            ],
            compiler_params=pltpu.CompilerParams(
                collective_id=0, has_side_effects=True, vmem_limit_bytes=64 * 1024 * 1024 - 2 * 1024 * 1024
            ),
            name="wave",
        )(pressure, pressure_old, speed, widths, sx, sy, sz, amp.T, rx, ry, rz)
        final, traces, energy = pl.pallas_call(
            store,
            out_shape=tuple(jax.ShapeDtypeStruct(shape, F32) for shape in shapes),
            in_specs=[pl.BlockSpec(memory_space=pltpu.VMEM)] * 3,
            out_specs=(pl.BlockSpec(memory_space=pltpu.HBM),) * 3,
            scratch_shapes=[pltpu.SemaphoreType.DMA((3,))],
            compiler_params=pltpu.CompilerParams(has_side_effects=True, vmem_limit_bytes=1024 * 1024),
            name="store",
        )(*held)
        return final, traces.T, energy.reshape(steps)

    in_specs = (P("gx", "gy", None),) * 3 + (P(),) * 8
    out_specs = (P("gx", "gy", None), P(), P())
    return jax.shard_map(per_device, mesh=mesh, in_specs=in_specs, out_specs=out_specs, check_vma=False)
```
